32 devices in a mesh: rows: 8 (over z, y), feat: 4 (over x, core).
Axes of the slice: x: 2, y: 2, z: 4, core: 2. Of those that a mesh axis runs over, the one named last changes fastest.
Arguments:
- bin_index: int32 [16384, 512], P('rows', 'feat'), may hold values from 0 to 255
- leaf_ids: int32 [16384], P('rows'), may hold values from 0 to 15
- gradients: bfloat16 [16384], P('rows'), may hold values from -3 to 3
- hessians: bfloat16 [16384], P('rows'), may hold values from 0.049804688 to 0.25
Outputs:
- split_gains: float32 [4, 128, 16, 256], P('feat', 'rows')
- best_gain: float32 [16], replicated
The draws below stay inside these ranges and needn't reach their ends.
All inputs are finite; a program needn't handle non-finite values.
Results may differ from the reference program's by a relative error of at most 0.0003.
Values may be sent and summed in bfloat16 or wider, within the bound.
A program may use at most 64 MiB of HBM per device.

```python
import math
import jax
import jax.numpy as jnp
import numpy as np
from jax import lax

FEATURES = 512
BINS = 256
LEAVES = 16
ROW_TOTAL = 16384
N_FEAT = 4


def touch_ends(entries, rng, low, high):
    longest = entries.shape.index(max(entries.shape))
    spots = []
    for shift in (0, 1):
        where = [jax.random.randint(jax.random.fold_in(rng, axis), (), 0, length) for axis, length in enumerate(entries.shape)]
        where[longest] = (where[longest] + shift) % entries.shape[longest]
        spots.append(tuple(where))
    return entries.at[spots[0]].set(low).at[spots[1]].set(high)


def block_levels(key, extent, cuts, low, top_value):
    factor_of, own = 1.0, jax.random.fold_in(key, 6)
    for position, shards_of in cuts:
        steps = jnp.exp(jax.random.uniform(jax.random.fold_in(own, position), (shards_of,), jnp.float32, low / len(cuts), top_value / len(cuts)))
        factor_of = factor_of * jnp.repeat(steps, extent[position] // shards_of).reshape([-1 if axis == position else 1 for axis in range(len(extent))])
    return factor_of


def cumulative_ranks(number_of, lean):
    loads = [(1 << 20) // math.isqrt(standing ** lean) + 1 for standing in range(1, number_of + 1)]
    width = 1 + sum(loads) // (1 << 30)
    return np.cumsum(np.array([max(1, weight // width) for weight in loads]))


def skewed_ids(own_key, shape, amount, lean):
    grid = cumulative_ranks(amount, lean)
    pick = jax.random.randint(jax.random.fold_in(own_key, 1), shape, 0, int(grid[amount - 1]))
    standing = jnp.searchsorted(jnp.asarray(grid, jnp.int32), pick, side="right")
    return jax.random.permutation(jax.random.fold_in(own_key, 2), amount)[standing].astype(jnp.int32)


def noise(stream_key, shape, spread, most, split=(), kind=jnp.bfloat16):
    loudness = block_levels(stream_key, shape, split, -0.22, 0.18) if split else 1.0
    result = jax.random.normal(stream_key, shape, jnp.float32) * spread * loudness
    return jnp.minimum(jnp.maximum(result, -most), most).astype(kind)


def setup_inputs(seed: int = 0) -> dict:
    arg_keys = jax.random.split(jax.random.key(seed), 5)
    return {
        "bin_index": touch_ends(jax.random.randint(arg_keys[0], (ROW_TOTAL, FEATURES), 0, BINS), jax.random.fold_in(arg_keys[0], 1), 0, BINS - 1).astype(jnp.int32),
        "leaf_ids": touch_ends(skewed_ids(arg_keys[1], (ROW_TOTAL,), LEAVES, 2), jax.random.fold_in(arg_keys[1], 3), 0, LEAVES - 1).astype(jnp.int32),
        "gradients": noise(arg_keys[2], (ROW_TOTAL,), 0.5, 3.0, ((0, 8),)),
        "hessians": jnp.clip(jnp.exp(math.log(0.25) - 1.6133518 * jax.random.uniform(arg_keys[3], (ROW_TOTAL,), jnp.float32) ** block_levels(arg_keys[3], (ROW_TOTAL,), ((0, 8),), -0.2, 0.2)), 0.049804688, 0.25).astype(jnp.bfloat16),
    }


reg_lambda = 1.0


def gain_of(left_grad, left_hess):
    total_grad = left_grad[:, :, -1:]
    total_hess = left_hess[:, :, -1:]
    right_grad = total_grad - left_grad
    right_hess = total_hess - left_hess
    return 0.5 * (left_grad * left_grad / (left_hess + reg_lambda)
                  + right_grad * right_grad / (right_hess + reg_lambda)
                  - total_grad * total_grad / (total_hess + reg_lambda))


def reference(bin_index, leaf_ids, gradients, hessians):
    grad_wide = gradients.astype(jnp.float32)
    hess_wide = hessians.astype(jnp.float32)
    group_width = math.gcd(FEATURES, 16)
    block_count = FEATURES // group_width
    segment_total = group_width * LEAVES * BINS

    def one_block(columns):
        offsets = jnp.arange(group_width, dtype=jnp.int32) * (LEAVES * BINS)
        flat_index = offsets[None, :] + leaf_ids[:, None] * BINS + columns
        flat_index = flat_index.reshape(-1)
        grad_flat = jnp.broadcast_to(grad_wide[:, None], columns.shape).reshape(-1)
        hess_flat = jnp.broadcast_to(hess_wide[:, None], columns.shape).reshape(-1)
        grad_hist = jax.ops.segment_sum(grad_flat, flat_index, num_segments=segment_total)
        hess_hist = jax.ops.segment_sum(hess_flat, flat_index, num_segments=segment_total)
        return (grad_hist.reshape(group_width, LEAVES, BINS), hess_hist.reshape(group_width, LEAVES, BINS))

    blocked = bin_index.reshape(ROW_TOTAL, block_count, group_width).transpose(1, 0, 2)
    hist_grad, hist_hess = lax.map(one_block, blocked)
    hist_grad = hist_grad.reshape(FEATURES, LEAVES, BINS)
    hist_hess = hist_hess.reshape(FEATURES, LEAVES, BINS)
    left_grad = jnp.cumsum(hist_grad, axis=2)
    left_hess = jnp.cumsum(hist_hess, axis=2)
    split_gains = gain_of(left_grad, left_hess)
    best_gain = jnp.max(split_gains, axis=(0, 2))
    return split_gains.reshape(N_FEAT, FEATURES // N_FEAT, LEAVES, BINS), best_gain
```

```python
import functools

import jax
import jax.numpy as jnp
from jax import lax
from jax.experimental import pallas as pl
from jax.experimental.pallas import tpu as pltpu
from jax.sharding import PartitionSpec as P

BINS = 256
LEAVES = 16
LANES = 128
HALF = BINS // 2
MESH = pl.DeviceIdType.MESH

reg_lambda = 1.0


def max_exchange(axis, count, source, landing, send_sems, recv_sems):
    me = lax.axis_index(axis)

    def copy_to(step):
        return pltpu.make_async_remote_copy(
            src_ref=source,
            dst_ref=landing.at[me],
            send_sem=send_sems.at[step],
            recv_sem=recv_sems.at[me],
            device_id={axis: lax.rem(me + step, count)},
            device_id_type=MESH,
        )

    def copy_from(step):
        origin = lax.rem(me - step + count, count)
        return origin, pltpu.make_async_remote_copy(
            src_ref=source,
            dst_ref=landing.at[origin],
            send_sem=send_sems.at[step],
            recv_sem=recv_sems.at[origin],
            device_id={axis: origin},
            device_id_type=MESH,
        )

    def start(step, carry):
        copy_to(step).start()
        return carry

    def collect(step, largest):
        origin, copy = copy_from(step)
        copy.wait_recv()
        return jnp.maximum(largest, landing[origin])

    def finish(step, carry):
        copy_to(step).wait_send()
        return carry

    lax.fori_loop(1, count, start, 0)
    largest = lax.fori_loop(1, count, collect, source[...])
    lax.fori_loop(1, count, finish, 0)
    return largest


def kernel(n, n_feat, group, bins_ref, meta_ref, gain_ref, best_ref, columns, metas, weights, sums,
           top_rows, top_feat, land_rows, land_feat,
           bin_send, bin_recv, meta_send, meta_recv, own_sems,
           row_send, row_recv, feat_send, feat_recv):
    me = lax.axis_index("rows")
    me_feat = lax.axis_index("feat")
    own, rows = bins_ref.shape[1], bins_ref.shape[2]
    tiles = rows // LANES

    barrier = pltpu.get_barrier_semaphore()

    def greet_rows(step, carry):
        pl.semaphore_signal(barrier, inc=1, device_id={"rows": lax.rem(me + step, n)}, device_id_type=MESH)
        return carry

    def greet_feat(step, carry):
        pl.semaphore_signal(barrier, inc=1, device_id={"feat": lax.rem(me_feat + step, n_feat)}, device_id_type=MESH)
        return carry

    lax.fori_loop(1, n, greet_rows, 0)
    lax.fori_loop(1, n_feat, greet_feat, 0)
    own_bins = pltpu.make_async_copy(bins_ref.at[me], columns.at[me], own_sems.at[0])
    own_meta = pltpu.make_async_copy(meta_ref, metas.at[me], own_sems.at[1])
    own_bins.start()
    own_meta.start()
    pl.semaphore_wait(barrier, n - 1 + n_feat - 1)

    def send(step):
        target = lax.rem(me + step, n)
        bins_copy = pltpu.make_async_remote_copy(
            src_ref=bins_ref.at[target], dst_ref=columns.at[me], send_sem=bin_send.at[step],
            recv_sem=bin_recv.at[me], device_id={"rows": target}, device_id_type=MESH)
        meta_copy = pltpu.make_async_remote_copy(
            src_ref=meta_ref, dst_ref=metas.at[me], send_sem=meta_send.at[step],
            recv_sem=meta_recv.at[me], device_id={"rows": target}, device_id_type=MESH)
        return bins_copy, meta_copy

    def receive(step):
        origin = lax.rem(me - step + n, n)
        bins_copy = pltpu.make_async_remote_copy(
            src_ref=bins_ref.at[origin], dst_ref=columns.at[origin], send_sem=bin_send.at[step],
            recv_sem=bin_recv.at[origin], device_id={"rows": origin}, device_id_type=MESH)
        meta_copy = pltpu.make_async_remote_copy(
            src_ref=meta_ref, dst_ref=metas.at[origin], send_sem=meta_send.at[step],
            recv_sem=meta_recv.at[origin], device_id={"rows": origin}, device_id_type=MESH)
        return bins_copy, meta_copy

    def start_sends(step, carry):
        for copy in send(step):
            copy.start()
        return carry

    lax.fori_loop(1, n, start_sends, 0)
    sums[...] = jnp.zeros_like(sums)
    own_bins.wait()
    own_meta.wait()

    def one_shard(step, carry):
        origin = lax.rem(me - step + n, n)

        @pl.when(step > 0)
        def arrived():
            for copy in receive(step):
                copy.wait_recv()

        table = metas[origin].astype(jnp.float32)
        leaf_of = lax.broadcasted_iota(jnp.int32, (LEAVES, LANES), 0).astype(jnp.float32)
        for tile in range(tiles):
            member = jnp.broadcast_to(table[tile:tile + 1], (LEAVES, LANES)) == leaf_of
            for part in (0, 1):
                first = (1 + part) * tiles + tile
                value = jnp.broadcast_to(table[first:first + 1], (LEAVES, LANES))
                weights[part * LEAVES:(part + 1) * LEAVES, tile * LANES:(tile + 1) * LANES] = (
                    jnp.where(member, value, 0.0).astype(jnp.bfloat16))

        block = columns[origin]
        level = lax.broadcasted_iota(jnp.int32, (HALF, rows), 0).astype(jnp.bfloat16)
        one, zero = jnp.ones((), jnp.bfloat16), jnp.zeros((), jnp.bfloat16)
        table_rows = weights[...]
        for first in range(0, own, group):
            left_side, right_side = [], []
            for feature in range(first, first + group):
                bins = block[feature:feature + 1]
                upper = bins >= HALF
                low = jnp.where(upper, bins - HALF, bins)
                upper_wide = jnp.broadcast_to(bins, (2 * LEAVES, rows)) >= HALF
                left_side.append(jnp.where(upper_wide, zero, table_rows))
                left_side.append(jnp.where(upper_wide, table_rows, zero))
                right_side.append(jnp.where(jnp.broadcast_to(low, (HALF, rows)) <= level, one, zero))
            product = lax.dot_general(
                jnp.concatenate(left_side, axis=0), jnp.concatenate(right_side, axis=0),
                (((1,), (1,)), ((), ())), preferred_element_type=jnp.float32)
            for place in range(group):
                sums[first + place] += product[place * 4 * LEAVES:(place + 1) * 4 * LEAVES, place * HALF:(place + 1) * HALF]
        return carry

    lax.fori_loop(0, n, one_shard, 0)

    def finish_sends(step, carry):
        for copy in send(step):
            copy.wait_send()
        return carry

    lax.fori_loop(1, n, finish_sends, 0)

    def gains(feature, largest):
        part = sums[feature]
        grad_low, hess_low = part[:LEAVES], part[LEAVES:2 * LEAVES]
        grad_high = part[2 * LEAVES:3 * LEAVES] + grad_low[:, HALF - 1:]
        hess_high = part[3 * LEAVES:] + hess_low[:, HALF - 1:]
        total_grad, total_hess = grad_high[:, HALF - 1:], hess_high[:, HALF - 1:]
        whole = total_grad * total_grad / (total_hess + reg_lambda)
        for place, left_grad, left_hess in ((0, grad_low, hess_low), (1, grad_high, hess_high)):
            right_grad, right_hess = total_grad - left_grad, total_hess - left_hess
            gain = 0.5 * (left_grad * left_grad / (left_hess + reg_lambda)
                          + right_grad * right_grad / (right_hess + reg_lambda) - whole)
            gain_ref[feature, :, place * HALF:(place + 1) * HALF] = gain
            largest = jnp.maximum(largest, gain)
        return largest

    top_rows[...] = lax.fori_loop(0, own, gains, jnp.full((LEAVES, HALF), -jnp.inf, jnp.float32))
    top_feat[...] = max_exchange("rows", n, top_rows, land_rows, row_send, row_recv)
    largest = max_exchange("feat", n_feat, top_feat, land_feat, feat_send, feat_recv)
    best_ref[...] = jnp.broadcast_to(jnp.max(largest, axis=1, keepdims=True), best_ref.shape)


def body(bin_index, leaf_ids, gradients, hessians):
    n, n_feat = lax.axis_size("rows"), lax.axis_size("feat")
    rows, local_features = bin_index.shape
    own = local_features // n
    group = 2 if own % 2 == 0 else 1
    bins = bin_index.T.astype(jnp.bfloat16).reshape(n, own, rows)
    meta = jnp.concatenate([leaf_ids.astype(jnp.bfloat16), gradients, hessians]).reshape(3 * rows // LANES, LANES)
    vmem = pl.BlockSpec(memory_space=pltpu.VMEM)
    dma = pltpu.SemaphoreType.DMA
    gain, best = pl.pallas_call(
        functools.partial(kernel, n, n_feat, group),
        out_shape=(jax.ShapeDtypeStruct((own, LEAVES, BINS), jnp.float32),
                   jax.ShapeDtypeStruct((LEAVES, LANES), jnp.float32)),
        in_specs=[vmem, vmem],
        out_specs=(vmem, vmem),
        scratch_shapes=[
            pltpu.VMEM((n, own, rows), jnp.bfloat16),
            pltpu.VMEM((n,) + meta.shape, jnp.bfloat16),
            pltpu.VMEM((2 * LEAVES, rows), jnp.bfloat16),
            pltpu.VMEM((own, 4 * LEAVES, HALF), jnp.float32),
            pltpu.VMEM((LEAVES, HALF), jnp.float32),
            pltpu.VMEM((LEAVES, HALF), jnp.float32),
            pltpu.VMEM((n, LEAVES, HALF), jnp.float32),
            pltpu.VMEM((n_feat, LEAVES, HALF), jnp.float32),
            dma((n,)), dma((n,)), dma((n,)), dma((n,)), dma((2,)),
            dma((n,)), dma((n,)), dma((n_feat,)), dma((n_feat,)),
        ],
        compiler_params=pltpu.CompilerParams(
            collective_id=0, has_side_effects=True, vmem_limit_bytes=60 * 1024 * 1024),
    )(bins, meta)
    return gain[None], best[:, 0]


def solution(mesh):
    placed = (P("rows", "feat"), P("rows"), P("rows"), P("rows"))
    return jax.shard_map(
        body,
        mesh=mesh,
        in_specs=placed,
        out_specs=(P("feat", "rows", None, None), P()),
        check_vma=False,
    )
```

```python
import functools

import jax
import jax.numpy as jnp
from jax import lax
from jax.experimental import pallas as pl
from jax.experimental.pallas import tpu as pltpu
from jax.sharding import PartitionSpec as P

BINS = 256
LEAVES = 16
LANES = 128
HALF = BINS // 2
MESH = pl.DeviceIdType.MESH

reg_lambda = 1.0


def kernel(n, n_feat, group, bins_hbm, leaf_ref, grad_ref, hess_ref, gain_ref, best_ref,
           raw, bins_src, meta_src, columns, metas, weights, sums, top, landing,
           raw_sems, bin_send, bin_recv, meta_send, meta_recv, own_sems, top_send, top_recv):
    me, me_feat = lax.axis_index("rows"), lax.axis_index("feat")
    everyone = n * n_feat
    me_all = me * n_feat + me_feat
    own, rows = bins_src.shape[1], bins_src.shape[2]
    tiles = rows // LANES
    pieces = raw_sems.shape[0]
    piece_rows = rows // pieces

    def fetch(piece):
        span = pl.ds(piece * piece_rows, piece_rows)
        return pltpu.make_async_copy(bins_hbm.at[span], raw.at[span], raw_sems.at[piece])

    for piece in range(pieces):
        fetch(piece).start()

    def device_after(step):
        other = lax.rem(me_all + step, everyone)
        return {"rows": other // n_feat, "feat": lax.rem(other, n_feat)}

    barrier = pltpu.get_barrier_semaphore()

    def greet(step, carry):
        pl.semaphore_signal(barrier, inc=1, device_id=device_after(step), device_id_type=MESH)
        return carry

    lax.fori_loop(1, everyone, greet, 0)

    meta_src[:tiles] = leaf_ref[...].astype(jnp.float32).astype(jnp.bfloat16)
    meta_src[tiles:2 * tiles] = grad_ref[...]
    meta_src[2 * tiles:] = hess_ref[...]
    for piece in range(pieces):
        fetch(piece).wait()
        for tile in range(piece * piece_rows // LANES, (piece + 1) * piece_rows // LANES):
            lanes = slice(tile * LANES, (tile + 1) * LANES)
            turned = raw[lanes].astype(jnp.float32).T.astype(jnp.bfloat16)
            bins_src[:, :, lanes] = turned.reshape(n, own, LANES)

    own_bins = pltpu.make_async_copy(bins_src.at[me], columns.at[me], own_sems.at[0])
    own_meta = pltpu.make_async_copy(meta_src, metas.at[me], own_sems.at[1])
    own_bins.start()
    own_meta.start()
    pl.semaphore_wait(barrier, everyone - 1)

    def partner(step):
        other, bit = 0, 1
        while bit < n:
            other += lax.rem(me // bit + step // bit, 2) * bit
            bit *= 2
        return other

    def exchange(step, landed):
        other = partner(step)
        place = other if landed else me
        copies = []
        for source, target, send_sems, recv_sems in (
                (meta_src, metas, meta_send, meta_recv), (bins_src.at[other], columns, bin_send, bin_recv)):
            copies.append(pltpu.make_async_remote_copy(
                src_ref=source, dst_ref=target.at[place], send_sem=send_sems.at[step],
                recv_sem=recv_sems.at[step], device_id={"rows": other}, device_id_type=MESH))
        return copies

    def start_sends(step, carry):
        for copy in exchange(step, False):
            copy.start()
        return carry

    lax.fori_loop(1, n, start_sends, 0)
    sums[...] = jnp.zeros_like(sums)
    own_bins.wait()
    own_meta.wait()

    def one_shard(step, carry):
        origin = partner(step)

        @pl.when(step > 0)
        def arrived():
            for copy in exchange(step, True):
                copy.wait_recv()

        table = metas[origin].astype(jnp.float32)
        leaf_of = lax.broadcasted_iota(jnp.int32, (LEAVES, LANES), 0).astype(jnp.float32)
        for tile in range(tiles):
            member = jnp.broadcast_to(table[tile:tile + 1], (LEAVES, LANES)) == leaf_of
            for part in (0, 1):
                first = (1 + part) * tiles + tile
                value = jnp.broadcast_to(table[first:first + 1], (LEAVES, LANES))
                weights[part * LEAVES:(part + 1) * LEAVES, tile * LANES:(tile + 1) * LANES] = (
                    jnp.where(member, value, 0.0).astype(jnp.bfloat16))

        block = columns[origin]
        level = lax.broadcasted_iota(jnp.int32, (HALF, rows), 0).astype(jnp.bfloat16)
        one, zero = jnp.ones((), jnp.bfloat16), jnp.zeros((), jnp.bfloat16)
        table_rows = weights[...]
        for first in range(0, own, group):
            left_side, right_side = [], []
            for feature in range(first, first + group):
                bins = block[feature:feature + 1]
                upper = bins >= HALF
                low = jnp.where(upper, bins - HALF, bins)
                upper_wide = jnp.broadcast_to(bins, (2 * LEAVES, rows)) >= HALF
                left_side.append(jnp.where(upper_wide, zero, table_rows))
                left_side.append(jnp.where(upper_wide, table_rows, zero))
                right_side.append(jnp.where(jnp.broadcast_to(low, (HALF, rows)) <= level, one, zero))
            product = lax.dot_general(
                jnp.concatenate(left_side, axis=0), jnp.concatenate(right_side, axis=0),
                (((1,), (1,)), ((), ())), preferred_element_type=jnp.float32)
            for place in range(group):
                sums[first + place] += product[place * 4 * LEAVES:(place + 1) * 4 * LEAVES, place * HALF:(place + 1) * HALF]
        return carry

    lax.fori_loop(0, n, one_shard, 0)

    def gains(feature, largest):
        part = sums[feature]
        grad_low, hess_low = part[:LEAVES], part[LEAVES:2 * LEAVES]
        grad_high = part[2 * LEAVES:3 * LEAVES] + grad_low[:, HALF - 1:]
        hess_high = part[3 * LEAVES:] + hess_low[:, HALF - 1:]
        total_grad, total_hess = grad_high[:, HALF - 1:], hess_high[:, HALF - 1:]
        whole = total_grad * total_grad / (total_hess + reg_lambda)
        for place, left_grad, left_hess in ((0, grad_low, hess_low), (1, grad_high, hess_high)):
            right_grad, right_hess = total_grad - left_grad, total_hess - left_hess
            gain = 0.5 * (left_grad * left_grad / (left_hess + reg_lambda)
                          + right_grad * right_grad / (right_hess + reg_lambda) - whole)
            gain_ref[feature, :, place * HALF:(place + 1) * HALF] = gain
            largest = jnp.maximum(largest, gain)
        return largest

    largest = lax.fori_loop(0, own, gains, jnp.full((LEAVES, HALF), -jnp.inf, jnp.float32))
    largest = jnp.broadcast_to(jnp.max(largest, axis=1, keepdims=True), (LEAVES, LANES))
    on_lane = (lax.broadcasted_iota(jnp.int32, (LEAVES, LANES), 0) == lax.broadcasted_iota(jnp.int32, (LEAVES, LANES), 1))
    top[...] = jnp.max(jnp.where(on_lane, largest, -jnp.inf), axis=0, keepdims=True)

    def report(step):
        return pltpu.make_async_remote_copy(
            src_ref=top, dst_ref=landing.at[step], send_sem=top_send.at[step],
            recv_sem=top_recv.at[step], device_id=device_after(step), device_id_type=MESH)

    def start_report(step, carry):
        report(step).start()
        return carry

    def collect(step, best):
        report(step).wait_recv()
        return jnp.maximum(best, landing[step])

    def finish(step, carry):
        report(step).wait_send()
        return carry

    def finish_sends(step, carry):
        for copy in exchange(step, False):
            copy.wait_send()
        return carry

    lax.fori_loop(1, everyone, start_report, 0)
    lax.fori_loop(1, n, finish_sends, 0)
    best = lax.fori_loop(1, everyone, collect, top[...])
    lax.fori_loop(1, everyone, finish, 0)
    best_ref[...] = best[:, :LEAVES]


def body(bin_index, leaf_ids, gradients, hessians):
    n, n_feat = lax.axis_size("rows"), lax.axis_size("feat")
    rows, local_features = bin_index.shape
    own = local_features // n
    group = 2 if own % 2 == 0 else 1
    tiles = rows // LANES
    pieces = 4
    everyone = n * n_feat
    vmem = pl.BlockSpec(memory_space=pltpu.VMEM)
    dma = pltpu.SemaphoreType.DMA
    gain, best = pl.pallas_call(
        functools.partial(kernel, n, n_feat, group),
        out_shape=(jax.ShapeDtypeStruct((own, LEAVES, BINS), jnp.float32),
                   jax.ShapeDtypeStruct((1, LEAVES), jnp.float32)),
        in_specs=[pl.BlockSpec(memory_space=pl.ANY), vmem, vmem, vmem],
        out_specs=(vmem, vmem),
        scratch_shapes=[
            pltpu.VMEM((rows, local_features), jnp.int32),
            pltpu.VMEM((n, own, rows), jnp.bfloat16),
            pltpu.VMEM((3 * tiles, LANES), jnp.bfloat16),
            pltpu.VMEM((n, own, rows), jnp.bfloat16),
            pltpu.VMEM((n, 3 * tiles, LANES), jnp.bfloat16),
            pltpu.VMEM((2 * LEAVES, rows), jnp.bfloat16),
            pltpu.VMEM((own, 4 * LEAVES, HALF), jnp.float32),
            pltpu.VMEM((1, LANES), jnp.float32),
            pltpu.VMEM((everyone, 1, LANES), jnp.float32),
            dma((pieces,)), dma((n,)), dma((n,)), dma((n,)), dma((n,)), dma((2,)),
            dma((everyone,)), dma((everyone,)),
        ],
        compiler_params=pltpu.CompilerParams(
            collective_id=0, has_side_effects=True, vmem_limit_bytes=60 * 1024 * 1024),
    )(bin_index, leaf_ids.reshape(tiles, LANES), gradients.reshape(tiles, LANES), hessians.reshape(tiles, LANES))
    return gain[None], best.reshape(LEAVES)


def solution(mesh):
    placed = (P("rows", "feat"), P("rows"), P("rows"), P("rows"))
    return jax.shard_map(
        body,
        mesh=mesh,
        in_specs=placed,
        out_specs=(P("feat", "rows", None, None), P()),
        check_vma=False,
    )
```

```python
import functools

import jax
import jax.numpy as jnp
from jax import lax
from jax.experimental import pallas as pl
from jax.experimental.pallas import tpu as pltpu
from jax.sharding import PartitionSpec as P

BINS = 256
LEAVES = 16
LANES = 128
HALF = BINS // 2
MESH = pl.DeviceIdType.MESH

reg_lambda = 1.0


def kernel(n, n_feat, group, bins_hbm, leaf_hbm, grad_hbm, hess_hbm, gain_ref, best_ref,
           leaf_ref, grad_ref, hess_ref, small_sems, raw, bins_src, meta_src, columns, metas, weights, sums, top, landing,
           raw_sems, bin_send, bin_recv, meta_send, meta_recv, own_sems, top_send, top_recv):
    me, me_feat = lax.axis_index("rows"), lax.axis_index("feat")
    everyone = n * n_feat
    me_all = me * n_feat + me_feat
    own, rows = bins_src.shape[1], bins_src.shape[2]
    tiles = rows // LANES
    pieces = raw_sems.shape[0]
    piece_rows = rows // pieces

    def fetch(piece):
        span = pl.ds(piece * piece_rows, piece_rows)
        return pltpu.make_async_copy(bins_hbm.at[span], raw.at[span], raw_sems.at[piece])

    small = [pltpu.make_async_copy(source, target, small_sems.at[place]) for place, (source, target) in enumerate(
        ((leaf_hbm, leaf_ref), (grad_hbm, grad_ref), (hess_hbm, hess_ref)))]
    for piece in range(pieces):
        fetch(piece).start()
    for copy in small:
        copy.start()

    def device_after(step):
        other = lax.rem(me_all + step, everyone)
        return {"rows": other // n_feat, "feat": lax.rem(other, n_feat)}

    barrier = pltpu.get_barrier_semaphore()

    def greet(step, carry):
        pl.semaphore_signal(barrier, inc=1, device_id=device_after(step), device_id_type=MESH)
        return carry

    lax.fori_loop(1, everyone, greet, 0)

    for copy in small:
        copy.wait()
    meta_src[:tiles] = leaf_ref[...].astype(jnp.float32).astype(jnp.bfloat16)
    meta_src[tiles:2 * tiles] = grad_ref[...]
    meta_src[2 * tiles:] = hess_ref[...]
    for piece in range(pieces):
        fetch(piece).wait()
        for tile in range(piece * piece_rows // LANES, (piece + 1) * piece_rows // LANES):
            lanes = slice(tile * LANES, (tile + 1) * LANES)
            turned = raw[lanes].astype(jnp.float32).T.astype(jnp.bfloat16)
            bins_src[:, :, lanes] = turned.reshape(n, own, LANES)

    own_bins = pltpu.make_async_copy(bins_src.at[me], columns.at[me], own_sems.at[0])
    own_meta = pltpu.make_async_copy(meta_src, metas.at[me], own_sems.at[1])
    own_bins.start()
    own_meta.start()
    pl.semaphore_wait(barrier, everyone - 1)

    def partner(step):
        other, bit = 0, 1
        while bit < n:
            other += lax.rem(me // bit + step // bit, 2) * bit
            bit *= 2
        return other

    def exchange(step, landed):
        other = partner(step)
        place = other if landed else me
        copies = []
        for source, target, send_sems, recv_sems in (
                (meta_src, metas, meta_send, meta_recv), (bins_src.at[other], columns, bin_send, bin_recv)):
            copies.append(pltpu.make_async_remote_copy(
                src_ref=source, dst_ref=target.at[place], send_sem=send_sems.at[step],
                recv_sem=recv_sems.at[step], device_id={"rows": other}, device_id_type=MESH))
        return copies

    def start_sends(step, carry):
        for copy in exchange(step, False):
            copy.start()
        return carry

    lax.fori_loop(1, n, start_sends, 0)
    sums[...] = jnp.zeros_like(sums)
    own_bins.wait()
    own_meta.wait()

    def one_shard(step, carry):
        origin = partner(step)

        @pl.when(step > 0)
        def arrived():
            for copy in exchange(step, True):
                copy.wait_recv()

        table = metas[origin].astype(jnp.float32)
        leaf_of = lax.broadcasted_iota(jnp.int32, (LEAVES, LANES), 0).astype(jnp.float32)
        for tile in range(tiles):
            member = jnp.broadcast_to(table[tile:tile + 1], (LEAVES, LANES)) == leaf_of
            for part in (0, 1):
                first = (1 + part) * tiles + tile
                value = jnp.broadcast_to(table[first:first + 1], (LEAVES, LANES))
                weights[part * LEAVES:(part + 1) * LEAVES, tile * LANES:(tile + 1) * LANES] = (
                    jnp.where(member, value, 0.0).astype(jnp.bfloat16))

        block = columns[origin]
        level = lax.broadcasted_iota(jnp.int32, (HALF, rows), 0).astype(jnp.bfloat16)
        one, zero = jnp.ones((), jnp.bfloat16), jnp.zeros((), jnp.bfloat16)
        table_rows = weights[...]
        for first in range(0, own, group):
            left_side, right_side = [], []
            for feature in range(first, first + group):
                bins = block[feature:feature + 1]
                upper = bins >= HALF
                low = jnp.where(upper, bins - HALF, bins)
                upper_wide = jnp.broadcast_to(bins, (2 * LEAVES, rows)) >= HALF
                left_side.append(jnp.where(upper_wide, zero, table_rows))
                left_side.append(jnp.where(upper_wide, table_rows, zero))
                right_side.append(jnp.where(jnp.broadcast_to(low, (HALF, rows)) <= level, one, zero).astype(jnp.float8_e4m3fn))
            product = lax.dot_general(
                jnp.concatenate(left_side, axis=0), jnp.concatenate(right_side, axis=0),
                (((1,), (1,)), ((), ())), preferred_element_type=jnp.float32)
            for place in range(group):
                sums[first + place] += product[place * 4 * LEAVES:(place + 1) * 4 * LEAVES, place * HALF:(place + 1) * HALF]
        return carry

    lax.fori_loop(0, n, one_shard, 0)

    def gains(feature, largest):
        part = sums[feature]
        grad_low, hess_low = part[:LEAVES], part[LEAVES:2 * LEAVES]
        grad_high = part[2 * LEAVES:3 * LEAVES] + grad_low[:, HALF - 1:]
        hess_high = part[3 * LEAVES:] + hess_low[:, HALF - 1:]
        total_grad, total_hess = grad_high[:, HALF - 1:], hess_high[:, HALF - 1:]
        whole = total_grad * total_grad / (total_hess + reg_lambda)
        for place, left_grad, left_hess in ((0, grad_low, hess_low), (1, grad_high, hess_high)):
            right_grad, right_hess = total_grad - left_grad, total_hess - left_hess
            gain = 0.5 * (left_grad * left_grad / (left_hess + reg_lambda)
                          + right_grad * right_grad / (right_hess + reg_lambda) - whole)
            gain_ref[feature, :, place * HALF:(place + 1) * HALF] = gain
            largest = jnp.maximum(largest, gain)
        return largest

    largest = lax.fori_loop(0, own, gains, jnp.full((LEAVES, HALF), -jnp.inf, jnp.float32), unroll=True)
    largest = jnp.broadcast_to(jnp.max(largest, axis=1, keepdims=True), (LEAVES, LANES))
    on_lane = (lax.broadcasted_iota(jnp.int32, (LEAVES, LANES), 0) == lax.broadcasted_iota(jnp.int32, (LEAVES, LANES), 1))
    top[...] = jnp.max(jnp.where(on_lane, largest, -jnp.inf), axis=0, keepdims=True)

    def report(step):
        return pltpu.make_async_remote_copy(
            src_ref=top, dst_ref=landing.at[step], send_sem=top_send.at[step],
            recv_sem=top_recv.at[step], device_id=device_after(step), device_id_type=MESH)

    def start_report(step, carry):
        report(step).start()
        return carry

    def collect(step, best):
        report(step).wait_recv()
        return jnp.maximum(best, landing[step])

    def finish(step, carry):
        report(step).wait_send()
        return carry

    def finish_sends(step, carry):
        for copy in exchange(step, False):
            copy.wait_send()
        return carry

    lax.fori_loop(1, everyone, start_report, 0)
    lax.fori_loop(1, n, finish_sends, 0)
    best = lax.fori_loop(1, everyone, collect, top[...])
    lax.fori_loop(1, everyone, finish, 0)
    best_ref[...] = best[:, :LEAVES]


def body(bin_index, leaf_ids, gradients, hessians):
    n, n_feat = lax.axis_size("rows"), lax.axis_size("feat")
    rows, local_features = bin_index.shape
    own = local_features // n
    group = 2 if own % 2 == 0 else 1
    tiles = rows // LANES
    pieces = 4
    everyone = n * n_feat
    vmem = pl.BlockSpec(memory_space=pltpu.VMEM)
    dma = pltpu.SemaphoreType.DMA
    gain, best = pl.pallas_call(
        functools.partial(kernel, n, n_feat, group),
        out_shape=(pltpu.VMEM((own, LEAVES, BINS), jnp.float32),
                   pltpu.VMEM((1, LEAVES), jnp.float32)),
        in_specs=[pl.BlockSpec(memory_space=pl.ANY)] * 4,
        out_specs=(vmem, vmem),
        scratch_shapes=[
            pltpu.VMEM((tiles, LANES), jnp.int32),
            pltpu.VMEM((tiles, LANES), jnp.bfloat16),
            pltpu.VMEM((tiles, LANES), jnp.bfloat16),
            dma((3,)),
            pltpu.VMEM((rows, local_features), jnp.int32),
            pltpu.VMEM((n, own, rows), jnp.bfloat16),
            pltpu.VMEM((3 * tiles, LANES), jnp.bfloat16),
            pltpu.VMEM((n, own, rows), jnp.bfloat16),
            pltpu.VMEM((n, 3 * tiles, LANES), jnp.bfloat16),
            pltpu.VMEM((2 * LEAVES, rows), jnp.bfloat16),
            pltpu.VMEM((own, 4 * LEAVES, HALF), jnp.float32),
            pltpu.VMEM((1, LANES), jnp.float32),
            pltpu.VMEM((everyone, 1, LANES), jnp.float32),
            dma((pieces,)), dma((n,)), dma((n,)), dma((n,)), dma((n,)), dma((2,)),
            dma((everyone,)), dma((everyone,)),
        ],
        compiler_params=pltpu.CompilerParams(
            collective_id=0, has_side_effects=True, vmem_limit_bytes=60 * 1024 * 1024),
    )(bin_index, leaf_ids.reshape(tiles, LANES), gradients.reshape(tiles, LANES), hessians.reshape(tiles, LANES))
    return gain[None], best.reshape(LEAVES)


def solution(mesh):
    placed = (P("rows", "feat"), P("rows"), P("rows"), P("rows"))
    return jax.shard_map(
        body,
        mesh=mesh,
        in_specs=placed,
        out_specs=(P("feat", "rows", None, None), P()),
        check_vma=False,
    )
```
